32 devices in a mesh: node: 4 (over x, core), sx: 2 (over y), sy: 4 (over z).
Axes of the slice: x: 2, y: 2, z: 4, core: 2. Of those that a mesh axis runs over, the one named last changes fastest.
Arguments:
- previous: float32 [4, 2, 32, 128, 256], P('node', None, 'sx', 'sy'), may hold values from 0 to 1
- feed_rate: float32 [32, 128, 256], P('sx', 'sy'), may hold values from 0.01 to 0.1
- kill_rate: float32 [32, 128, 256], P('sx', 'sy'), may hold values from 0.03 to 0.1
Outputs:
- sections: float32 [4, 2, 32, 128, 256], P('node', None, 'sx', 'sy')
The draws below stay inside these ranges and needn't reach their ends.
All inputs are finite; a program needn't handle non-finite values.
Results may differ from the reference program's by a relative error of at most 0.00011.
Values sent between devices are 32-bit elements; how exact they have to be, the bound alone decides.
A program may use at most 64 MiB of HBM per device.

```python
import math
import jax
import jax.numpy as jnp
from jax import lax

M = 4
SPECIES = 2
SWEEPS = 2
JACOBI = 12
NZ = 256
NX = 32
NY = 128


def draw_previous(key, part):
    local_key = jax.random.fold_in(key, 7301)
    first_index = jnp.arange(NX, dtype=jnp.int32)[:, None, None]
    second_index = jnp.arange(NY, dtype=jnp.int32)[None, :, None]
    third_index = jnp.arange(NZ, dtype=jnp.int32)[None, None, :]
    parity = (first_index + second_index + third_index) % 2
    pattern = (1 - 2 * parity).astype(jnp.float32)
    uniform_part = jax.random.uniform(local_key, (M, SPECIES, NX, NY, NZ), jnp.float32)
    factor = 0.5 + 0.5 * uniform_part
    values = 0.5 + 0.49 * factor * pattern[None, None]
    return values.astype(jnp.float32)


def levels(key, dims, split, least, top_value):
    def one(axis_at, parts):
        heights = jax.random.uniform(jax.random.fold_in(jax.random.fold_in(key, 6), axis_at), (parts,), jnp.float32, least / len(split), top_value / len(split))
        return jnp.repeat(jnp.exp(heights), dims[axis_at] // parts).reshape((-1,) + (1,) * (len(dims) - axis_at - 1))

    loudness = one(*split[0])
    for cut in split[1:]:
        loudness = loudness * one(*cut)
    return loudness


def setup_inputs(seed: int = 0) -> dict:
    key_of = jax.random.split(jax.random.key(seed), 4)
    previous = draw_previous(jax.random.fold_in(key_of[3], 71), 0)
    feed_rate = jnp.clip(jnp.exp(math.log(0.1) - 2.3025851 * jax.random.uniform(key_of[1], (NX, NY, NZ), jnp.float32) ** levels(key_of[1], (NX, NY, NZ), ((0, 2), (1, 4)), -0.2, 0.2)), 0.01, 0.1)
    kill_rate = jnp.clip(jnp.exp(math.log(0.1) - 1.2039728 * jax.random.uniform(key_of[2], (NX, NY, NZ), jnp.float32) ** levels(key_of[2], (NX, NY, NZ), ((0, 2), (1, 4)), -0.2, 0.2)), 0.03, 0.1)
    return {"previous": previous, "feed_rate": feed_rate, "kill_rate": kill_rate}


radau_points = [0.088587959512704, 0.409466864440735, 0.787659461760847, 1.0]
time_step = 4.0
diffusion_values = [1.0, 0.5]


def collocation():
    count = len(radau_points)
    table = []
    for row in range(count):
        table.append([0.0] * count)
    for column in range(count):
        poly = [1.0]
        denom = 1.0
        for other in range(count):
            if other != column:
                longer = [0.0] * (len(poly) + 1)
                for place in range(len(poly)):
                    longer[place + 1] = longer[place + 1] + poly[place]
                    longer[place] = longer[place] - radau_points[other] * poly[place]
                poly = longer
                denom = denom * (radau_points[column] - radau_points[other])
        for row in range(count):
            point = radau_points[row]
            total = 0.0
            for place in range(len(poly)):
                total = total + poly[place] * point ** (place + 1) / (place + 1)
            table[row][column] = total / denom
    return table


def neighbours(field):
    total = jnp.roll(field, 1, 2) + jnp.roll(field, -1, 2)
    total = total + jnp.roll(field, 1, 3) + jnp.roll(field, -1, 3)
    return total + jnp.roll(field, 1, 4) + jnp.roll(field, -1, 4)


def reaction(field, feed_rate, kill_rate):
    upart = field[:, 0]
    vpart = field[:, 1]
    uvv = upart * vpart * vpart
    first = -uvv + feed_rate[None] * (1.0 - upart)
    second = uvv - (feed_rate[None] + kill_rate[None]) * vpart
    return jnp.stack([first, second], 1)


def reference(previous, feed_rate, kill_rate):
    qmatrix = jnp.asarray(collocation(), jnp.float32)
    points = jnp.asarray(radau_points, jnp.float32)[:, None, None, None, None]
    diffusion = jnp.asarray(diffusion_values, jnp.float32)[None, :, None, None, None]
    coef = time_step * points * diffusion
    start_value = previous[-1]
    iterate = previous
    for sweep in range(SWEEPS):
        laplace = neighbours(iterate) - 6.0 * iterate
        diff = diffusion * laplace
        force = diff + reaction(iterate, feed_rate, kill_rate)
        summed = jnp.einsum("mj,jsxyz->msxyz", qmatrix, force, precision=lax.Precision.HIGHEST)
        right_side = start_value[None] + time_step * (summed - points * diff)

        def jacobi(turn, current):
            return (right_side + coef * neighbours(current)) / (1.0 + 6.0 * coef)

        iterate = lax.fori_loop(0, JACOBI, jacobi, iterate)
    return iterate
```

```python
import jax
import jax.numpy as jnp
from jax import lax
from jax.experimental import pallas as pl
from jax.experimental.pallas import tpu as pltpu
from jax.sharding import PartitionSpec as P

MESH = pl.DeviceIdType.MESH
WIDTH = 4
CHUNKS = 4

SWEEPS = 2
JACOBI = 12


radau_points = [0.088587959512704, 0.409466864440735, 0.787659461760847, 1.0]
time_step = 4.0
diffusion_values = [1.0, 0.5]


def from_root(value, axis, source):
    kept = jnp.where(lax.axis_index(axis) == source, value, 0).astype(value.dtype)
    return lax.psum(kept, axis)


def padded_2(block, sides, width):
    for axis, dim in sides:
        count = lax.axis_size(axis)
        forward = [(i, i + 1) for i in range(count - 1)]
        forward.append((count - 1, 0))
        backward = [(target, source) for source, target in forward]
        low = lax.ppermute(
            lax.slice_in_dim(block, block.shape[dim] - width, None, axis=dim), axis, forward
        )
        high = lax.ppermute(lax.slice_in_dim(block, 0, width, axis=dim), axis, backward)
        block = jnp.concatenate([low, block, high], axis=dim)
    return block


def collocation():
    count = len(radau_points)
    table = []
    for row in range(count):
        table.append([0.0] * count)
    for column in range(count):
        poly = [1.0]
        denom = 1.0
        for other in range(count):
            if other != column:
                longer = [0.0] * (len(poly) + 1)
                for place in range(len(poly)):
                    longer[place + 1] = longer[place + 1] + poly[place]
                    longer[place] = longer[place] - radau_points[other] * poly[place]
                poly = longer
                denom = denom * (radau_points[column] - radau_points[other])
        for row in range(count):
            point = radau_points[row]
            total = 0.0
            for place in range(len(poly)):
                total = total + poly[place] * point ** (place + 1) / (place + 1)
            table[row][column] = total / denom
    return table


def beside(padded):
    center = padded[:, 1:-1, 1:-1]
    total = padded[:, 2:, 1:-1] + padded[:, :-2, 1:-1]
    total = total + padded[:, 1:-1, 2:] + padded[:, 1:-1, :-2]
    return total + jnp.roll(center, 1, 3) + jnp.roll(center, -1, 3)


def body(previous, feed_rate, kill_rate):
    node_index = lax.axis_index("node")
    qmatrix = jnp.asarray(collocation(), jnp.float32)
    points = jnp.asarray(radau_points, jnp.float32)
    diag_weight = points[node_index]
    diffusion = jnp.asarray(diffusion_values, jnp.float32)[:, None, None, None]
    coef = time_step * diag_weight * diffusion
    start_value = from_root(previous[0], "node", len(radau_points) - 1)
    iterate = previous[0]
    for sweep in range(SWEEPS):
        padded = padded_2(iterate, (("sx", 1), ("sy", 2)), 1)
        diff = diffusion * (beside(padded) - 6.0 * iterate)
        upart = iterate[0]
        vpart = iterate[1]
        uvv = upart * vpart * vpart
        react = jnp.stack(
            [-uvv + feed_rate * (1.0 - upart), uvv - (feed_rate + kill_rate) * vpart], 0
        )
        force = diff + react
        weights = qmatrix[:, node_index][:, None, None, None, None]
        section_terms = weights * force[None]
        summed = lax.psum_scatter(section_terms, "node", scatter_dimension=0, tiled=True)[0]
        right_side = start_value + time_step * (summed - diag_weight * diff)
        extended = padded_2(right_side, (("sx", 1), ("sy", 2)), 1)

        def double_turn(turn, current):
            beside_all = padded_2(current, (("sx", 1), ("sy", 2)), 2)
            midway = (extended + coef * beside(beside_all)) / (1.0 + 6.0 * coef)
            return (right_side + coef * beside(midway)) / (1.0 + 6.0 * coef)

        iterate = lax.fori_loop(0, JACOBI // 2, double_turn, iterate)
    return iterate[None]


def pick(values, index):
    out = jnp.float32(values[-1])
    for at in range(len(values) - 1):
        out = jnp.where(index == at, jnp.float32(values[at]), out)
    return out


def pick_pair(table, row, column):
    out = pick(table[-1], column)
    for at in range(len(table) - 1):
        out = jnp.where(row == at, pick(table[at], column), out)
    return out


def kernel(
    sy_count, x_ref, f_ref, k_ref, out_ref,
    xe, edge_out, edge_in, diff, force, force_in, start, part_out, part_in,
    local, right_out, rj, xj, halo_out, halo_in, back, send_sems, recv_sems,
):
    w = WIDTH
    _, ny, nx, nz = x_ref.shape
    full = 2 * nx
    step = ny // CHUNKS
    m, s, t = lax.axis_index("node"), lax.axis_index("sx"), lax.axis_index("sy")
    other = 1 - s
    core = {"node": m + 1 - 2 * lax.rem(m, 2)}
    across = {"node": lax.rem(m + 2, 4)}
    pair = {"sx": other}
    up = {"sy": lax.rem(t + 1, sy_count)}
    down = {"sy": lax.rem(t + sy_count - 1, sy_count)}
    m1, m2 = core["node"], across["node"]
    count = [0]

    def send(src, dst, target):
        at = count[0]
        count[0] += 1
        copy = pltpu.make_async_remote_copy(
            src_ref=src, dst_ref=dst, send_sem=send_sems.at[at], recv_sem=recv_sems.at[at],
            device_id=target, device_id_type=MESH,
        )
        copy.start()
        started.append(copy)
        return copy

    started = []
    barrier = pltpu.get_barrier_semaphore()
    for target in (core, across, pair, up, down):
        pl.semaphore_signal(barrier, inc=1, device_id=target, device_id_type=MESH)

    table = collocation()
    h = time_step
    q_own, q_core = h * pick_pair(table, m, m), h * pick_pair(table, m, m1)
    p_own, p_core = h * pick_pair(table, m2, m), h * pick_pair(table, m2, m1)
    tau = pick(radau_points, m)
    has_start = jnp.where(m >= 2, jnp.float32(1.0), jnp.float32(0.0))
    scale = [1.0 / (1.0 + 6.0 * h * tau * d) for d in diffusion_values]
    coef_s = h * tau * pick(diffusion_values, s)
    gain = coef_s / (1.0 + 6.0 * coef_s)
    own_rows = pl.ds(pl.multiple_of(nx * s, nx), nx)
    other_rows = pl.ds(pl.multiple_of(nx * other, nx), nx)
    row = lax.broadcasted_iota(jnp.int32, (nx, nz), 0)

    def planes(first, last, fn, unroll=1):
        def go(y, carry):
            fn(y)
            return carry
        if last > first:
            lax.fori_loop(first, last, go, 0, unroll=unroll)

    def load(y):
        for a in range(2):
            xe[0, a, y + 1] = x_ref[a, y]
        xj[0, y + w, own_rows, :] = x_ref[s, y]

    planes(0, ny, load)
    pl.semaphore_wait(barrier, 5)

    exchanges = 0
    first_pair = None
    for sweep in range(SWEEPS):
        x = xe.at[sweep]

        def edges(y):
            for a in range(2):
                edge_out[sweep, 0, a, pl.ds(y, 1), :] = x[a, y + 1, pl.ds(0, 1), :]
                edge_out[sweep, 1, a, pl.ds(y, 1), :] = x[a, y + 1, pl.ds(nx - 1, 1), :]

        edge_copies = [
            send(x.at[:, ny], x.at[:, 0], up),
            send(x.at[:, 1], x.at[:, ny + 1], down),
        ]
        planes(0, ny, edges)
        edge_copies += [
            send(edge_out.at[sweep, 1], edge_in.at[sweep, 0], pair),
            send(edge_out.at[sweep, 0], edge_in.at[sweep, 1], pair),
        ]
        start_copy = None
        if sweep == 0:
            start_copy = send(x_ref, start, core)
            first_pair = send(x_ref.at[other], xj.at[0, pl.ds(w, ny), own_rows, :], pair)
        for copy in edge_copies:
            copy.wait_recv()

        def forces(y):
            u, v = x[0, y + 1], x[1, y + 1]
            feed, kill = f_ref[y], k_ref[y]
            uvv = u * v * v
            react = (feed * (1.0 - u) - uvv, uvv - (feed + kill) * v)
            for a, value in enumerate((u, v)):
                low = edge_in[sweep, 0, a, pl.ds(y, 1), :]
                high = edge_in[sweep, 1, a, pl.ds(y, 1), :]
                total = x[a, y] + x[a, y + 2]
                total = total + jnp.where(row == 0, low, pltpu.roll(value, 1, 0))
                total = total + jnp.where(row == nx - 1, high, pltpu.roll(value, nx - 1, 0))
                total = total + pltpu.roll(value, 1, 1) + pltpu.roll(value, nz - 1, 1)
                d = diffusion_values[a] * (total - 6.0 * value)
                diff[a, y] = d
                force[sweep, a, y] = d + react[a]

        order = [0, CHUNKS - 1] + list(range(1, CHUNKS - 1))
        core_copies, part_copies, right_copies = {}, {}, {}
        for c in order:
            rows = pl.ds(c * step, step)
            planes(c * step, (c + 1) * step, forces)
            core_copies[c] = send(
                force.at[sweep, :, rows], force_in.at[sweep, :, rows], core
            )
        if sweep == 0:
            start_copy.wait_recv()

            def begin(y):
                for a in range(2):
                    first = jnp.where(lax.rem(m, 2) == 1, x_ref[a, y], start[a, y])
                    start_kept[a, y] = has_start * first

            start_kept = local.at[1]
            planes(0, ny, begin)
        start_kept = local.at[1]

        def parts(y):
            for a in range(2):
                f, g, begin_value = force[sweep, a, y], force_in[sweep, a, y], start_kept[a, y]
                part_out[sweep, a, y] = begin_value + p_own * f + p_core * g
                local[0, a, y] = begin_value + q_own * f + q_core * g - (h * tau) * diff[a, y]

        for c in order:
            rows = pl.ds(c * step, step)
            core_copies[c].wait_recv()
            planes(c * step, (c + 1) * step, parts)
            part_copies[c] = send(
                part_out.at[sweep, :, rows], part_in.at[sweep, :, rows], across
            )

        scale_own = jnp.where(s == 0, scale[0], scale[1])
        scale_other = jnp.where(s == 0, scale[1], scale[0])

        def rights(y):
            rj[sweep, y + w, own_rows, :] = (local[0, s, y] + part_in[sweep, s, y]) * scale_own
            right_out[sweep, y] = (local[0, other, y] + part_in[sweep, other, y]) * scale_other

        for c in order:
            part_copies[c].wait_recv()
            planes(c * step, (c + 1) * step, rights)
            right_copies[c] = send(
                right_out.at[sweep, pl.ds(c * step, step)],
                rj.at[sweep, pl.ds(w + c * step, step), own_rows, :],
                pair,
            )
        if sweep == 0:
            first_pair.wait_recv()
        for c in order[:2]:
            right_copies[c].wait_recv()
        right_halo = [
            send(rj.at[sweep, pl.ds(w, w - 1)], rj.at[sweep, pl.ds(w + ny, w - 1)], down),
            send(rj.at[sweep, pl.ds(w + ny - w + 1, w - 1)], rj.at[sweep, pl.ds(1, w - 1)], up),
        ]
        for block in range(JACOBI // w):
            e = exchanges
            exchanges += 1
            for y in range(w):
                halo_out[e, 0, y] = xj[0, w + y]
                halo_out[e, 1, y] = xj[0, ny + y]
            copies = [
                send(halo_out.at[e, 0], halo_in.at[e, 0], down),
                send(halo_out.at[e, 1], halo_in.at[e, 1], up),
            ]
            if block == 0:
                for c in order[2:]:
                    right_copies[c].wait_recv()

            def sweep_planes(turn, first, last):
                src, dst = (turn - 1) % 2, turn % 2

                def one(y):
                    value = xj[src, y]
                    total = xj[src, y - 1] + xj[src, y + 1]
                    total = total + pltpu.roll(value, 1, 0) + pltpu.roll(value, full - 1, 0)
                    total = total + pltpu.roll(value, 1, 1) + pltpu.roll(value, nz - 1, 1)
                    xj[dst, y] = rj[sweep, y] + gain * total

                planes(first + w, last + w, one)

            for turn in range(1, w + 1):
                sweep_planes(turn, turn, ny - turn)
            for copy in copies:
                copy.wait_recv()
            if block == 0:
                for copy in right_halo:
                    copy.wait_recv()
            for y in range(w):
                xj[0, w + ny + y] = halo_in[e, 0, y]
                xj[0, y] = halo_in[e, 1, y]
            for turn in range(1, w + 1):
                sweep_planes(turn, turn - w, turn)
                sweep_planes(turn, ny - turn, ny + w - turn)
        source = xj.at[0, pl.ds(w, ny), other_rows, :]
        if sweep < SWEEPS - 1:
            copy = send(source, xe.at[sweep + 1, s, pl.ds(1, ny)], pair)

            def keep(y):
                xe[sweep + 1, s, y + 1] = xj[0, y + w, own_rows, :]

            planes(0, ny, keep)
            copy.wait_recv()
            copy.wait_send()
            started.pop()
        else:
            copy = send(source, back, pair)

            def keep(y):
                out_ref[s, y] = xj[0, y + w, own_rows, :]

            planes(0, ny, keep)
            copy.wait_recv()

            def finish(y):
                out_ref[other, y] = back[y]

            planes(0, ny, finish)
    for copy in started:
        copy.wait_send()


def fast_body(sy_count, previous, feed_rate, kill_rate):
    f32 = jnp.float32
    x = jnp.swapaxes(previous[0], 1, 2)
    _, ny, nx, nz = x.shape
    w = WIDTH
    block = (2, ny, nx, nz)
    blocks = SWEEPS * (JACOBI // w)
    copies = SWEEPS * (4 + 3 * CHUNKS + 2 + 2 * (JACOBI // w) + 1) + 2
    vmem = pl.BlockSpec(memory_space=pltpu.VMEM)
    out = pl.pallas_call(
        lambda *refs: kernel(sy_count, *refs),
        out_shape=jax.ShapeDtypeStruct(block, f32),
        in_specs=[vmem] * 3,
        out_specs=vmem,
        scratch_shapes=[
            pltpu.VMEM((SWEEPS, 2, ny + 2, nx, nz), f32),
            pltpu.VMEM((SWEEPS, 2, 2, ny, nz), f32),
            pltpu.VMEM((SWEEPS, 2, 2, ny, nz), f32),
            pltpu.VMEM(block, f32),
            pltpu.VMEM((SWEEPS,) + block, f32),
            pltpu.VMEM((SWEEPS,) + block, f32),
            pltpu.VMEM(block, f32),
            pltpu.VMEM((SWEEPS,) + block, f32),
            pltpu.VMEM((SWEEPS,) + block, f32),
            pltpu.VMEM((2,) + block, f32),
            pltpu.VMEM((SWEEPS, ny, nx, nz), f32),
            pltpu.VMEM((SWEEPS, ny + 2 * w, 2 * nx, nz), f32),
            pltpu.VMEM((2, ny + 2 * w, 2 * nx, nz), f32),
            pltpu.VMEM((blocks, 2, w, 2 * nx, nz), f32),
            pltpu.VMEM((blocks, 2, w, 2 * nx, nz), f32),
            pltpu.VMEM((ny, nx, nz), f32),
            pltpu.SemaphoreType.DMA((copies,)),
            pltpu.SemaphoreType.DMA((copies,)),
        ],
        compiler_params=pltpu.CompilerParams(
            collective_id=0, has_side_effects=True, vmem_limit_bytes=48 * 1024 * 1024
        ),
    )(x, jnp.swapaxes(feed_rate, 0, 1), jnp.swapaxes(kill_rate, 0, 1))
    return jnp.swapaxes(out, 1, 2)[None]


def solution(mesh):
    sizes = dict(mesh.shape)
    fast = sizes["sx"] == 2 and sizes["node"] == len(radau_points) and sizes["sy"] > 2

    def run(previous, feed_rate, kill_rate):
        if fast:
            return fast_body(sizes["sy"], previous, feed_rate, kill_rate)
        return body(previous, feed_rate, kill_rate)

    return jax.shard_map(
        run,
        mesh=mesh,
        in_specs=(P("node", None, "sx", "sy", None), P("sx", "sy", None), P("sx", "sy", None)),
        out_specs=P("node", None, "sx", "sy", None),
        check_vma=False,
    )
```

```python
import jax
import jax.numpy as jnp
from jax import lax
from jax.experimental import pallas as pl
from jax.experimental.pallas import tpu as pltpu
from jax.sharding import PartitionSpec as P

MESH = pl.DeviceIdType.MESH
WIDTH = 12
CHUNKS = 4

SWEEPS = 2
JACOBI = 12


radau_points = [0.088587959512704, 0.409466864440735, 0.787659461760847, 1.0]
time_step = 4.0
diffusion_values = [1.0, 0.5]


def from_root(value, axis, source):
    kept = jnp.where(lax.axis_index(axis) == source, value, 0).astype(value.dtype)
    return lax.psum(kept, axis)


def padded_2(block, sides, width):
    for axis, dim in sides:
        count = lax.axis_size(axis)
        forward = [(i, i + 1) for i in range(count - 1)]
        forward.append((count - 1, 0))
        backward = [(target, source) for source, target in forward]
        low = lax.ppermute(
            lax.slice_in_dim(block, block.shape[dim] - width, None, axis=dim), axis, forward
        )
        high = lax.ppermute(lax.slice_in_dim(block, 0, width, axis=dim), axis, backward)
        block = jnp.concatenate([low, block, high], axis=dim)
    return block


def collocation():
    count = len(radau_points)
    table = []
    for row in range(count):
        table.append([0.0] * count)
    for column in range(count):
        poly = [1.0]
        denom = 1.0
        for other in range(count):
            if other != column:
                longer = [0.0] * (len(poly) + 1)
                for place in range(len(poly)):
                    longer[place + 1] = longer[place + 1] + poly[place]
                    longer[place] = longer[place] - radau_points[other] * poly[place]
                poly = longer
                denom = denom * (radau_points[column] - radau_points[other])
        for row in range(count):
            point = radau_points[row]
            total = 0.0
            for place in range(len(poly)):
                total = total + poly[place] * point ** (place + 1) / (place + 1)
            table[row][column] = total / denom
    return table


def beside(padded):
    center = padded[:, 1:-1, 1:-1]
    total = padded[:, 2:, 1:-1] + padded[:, :-2, 1:-1]
    total = total + padded[:, 1:-1, 2:] + padded[:, 1:-1, :-2]
    return total + jnp.roll(center, 1, 3) + jnp.roll(center, -1, 3)


def body(previous, feed_rate, kill_rate):
    node_index = lax.axis_index("node")
    qmatrix = jnp.asarray(collocation(), jnp.float32)
    points = jnp.asarray(radau_points, jnp.float32)
    diag_weight = points[node_index]
    diffusion = jnp.asarray(diffusion_values, jnp.float32)[:, None, None, None]
    coef = time_step * diag_weight * diffusion
    start_value = from_root(previous[0], "node", len(radau_points) - 1)
    iterate = previous[0]
    for sweep in range(SWEEPS):
        padded = padded_2(iterate, (("sx", 1), ("sy", 2)), 1)
        diff = diffusion * (beside(padded) - 6.0 * iterate)
        upart = iterate[0]
        vpart = iterate[1]
        uvv = upart * vpart * vpart
        react = jnp.stack(
            [-uvv + feed_rate * (1.0 - upart), uvv - (feed_rate + kill_rate) * vpart], 0
        )
        force = diff + react
        weights = qmatrix[:, node_index][:, None, None, None, None]
        section_terms = weights * force[None]
        summed = lax.psum_scatter(section_terms, "node", scatter_dimension=0, tiled=True)[0]
        right_side = start_value + time_step * (summed - diag_weight * diff)
        extended = padded_2(right_side, (("sx", 1), ("sy", 2)), 1)

        def double_turn(turn, current):
            beside_all = padded_2(current, (("sx", 1), ("sy", 2)), 2)
            midway = (extended + coef * beside(beside_all)) / (1.0 + 6.0 * coef)
            return (right_side + coef * beside(midway)) / (1.0 + 6.0 * coef)

        iterate = lax.fori_loop(0, JACOBI // 2, double_turn, iterate)
    return iterate[None]


def pick(values, index):
    out = jnp.float32(values[-1])
    for at in range(len(values) - 1):
        out = jnp.where(index == at, jnp.float32(values[at]), out)
    return out


def pick_pair(table, row, column):
    out = pick(table[-1], column)
    for at in range(len(table) - 1):
        out = jnp.where(row == at, pick(table[at], column), out)
    return out


def kernel(
    sy_count, x_ref, f_ref, k_ref, out_ref,
    xe, edge_out, edge_in, diff, force, force_in, start, part_out, part_in,
    local, right_out, rj, xj, halo_out, halo_in, back, send_sems, recv_sems,
):
    w = WIDTH
    _, ny, nx, nz = x_ref.shape
    full = 2 * nx
    step = ny // CHUNKS
    m, s, t = lax.axis_index("node"), lax.axis_index("sx"), lax.axis_index("sy")
    other = 1 - s
    core = {"node": m + 1 - 2 * lax.rem(m, 2)}
    across = {"node": lax.rem(m + 2, 4)}
    pair = {"sx": other}
    up = {"sy": lax.rem(t + 1, sy_count)}
    down = {"sy": lax.rem(t + sy_count - 1, sy_count)}
    m1, m2 = core["node"], across["node"]
    count = [0]

    def send(src, dst, target):
        at = count[0]
        count[0] += 1
        copy = pltpu.make_async_remote_copy(
            src_ref=src, dst_ref=dst, send_sem=send_sems.at[at], recv_sem=recv_sems.at[at],
            device_id=target, device_id_type=MESH,
        )
        copy.start()
        started.append(copy)
        return copy

    started = []
    barrier = pltpu.get_barrier_semaphore()
    for target in (core, across, pair, up, down):
        pl.semaphore_signal(barrier, inc=1, device_id=target, device_id_type=MESH)

    table = collocation()
    h = time_step
    q_own, q_core = h * pick_pair(table, m, m), h * pick_pair(table, m, m1)
    p_own, p_core = h * pick_pair(table, m2, m), h * pick_pair(table, m2, m1)
    tau = pick(radau_points, m)
    has_start = jnp.where(m >= 2, jnp.float32(1.0), jnp.float32(0.0))
    scale = [1.0 / (1.0 + 6.0 * h * tau * d) for d in diffusion_values]
    coef_s = h * tau * pick(diffusion_values, s)
    gain = coef_s / (1.0 + 6.0 * coef_s)
    own_rows = pl.ds(pl.multiple_of(nx * s, nx), nx)
    other_rows = pl.ds(pl.multiple_of(nx * other, nx), nx)
    row = lax.broadcasted_iota(jnp.int32, (nx, nz), 0)

    def planes(first, last, fn, unroll=1):
        def go(y, carry):
            fn(y)
            return carry
        if last > first:
            lax.fori_loop(first, last, go, 0, unroll=unroll)

    def load(y):
        for a in range(2):
            xe[0, a, y + 1] = x_ref[a, y]
        xj[0, y + w, own_rows, :] = x_ref[s, y]

    planes(0, ny, load)
    pl.semaphore_wait(barrier, 5)

    exchanges = 0
    first_pair = None
    for sweep in range(SWEEPS):
        x = xe.at[sweep]

        def edges(y):
            for a in range(2):
                edge_out[sweep, 0, a, pl.ds(y, 1), :] = x[a, y + 1, pl.ds(0, 1), :]
                edge_out[sweep, 1, a, pl.ds(y, 1), :] = x[a, y + 1, pl.ds(nx - 1, 1), :]

        edge_copies = [
            send(x.at[:, ny], x.at[:, 0], up),
            send(x.at[:, 1], x.at[:, ny + 1], down),
        ]
        planes(0, ny, edges)
        edge_copies += [
            send(edge_out.at[sweep, 1], edge_in.at[sweep, 0], pair),
            send(edge_out.at[sweep, 0], edge_in.at[sweep, 1], pair),
        ]
        start_copy = None
        if sweep == 0:
            start_copy = send(x_ref, start, core)
            first_pair = send(x_ref.at[other], xj.at[0, pl.ds(w, ny), own_rows, :], pair)
        for copy in edge_copies:
            copy.wait_recv()

        def send_halo(e):
            def stage(y):
                halo_out[e, 0, y] = xj[0, w + y]
                halo_out[e, 1, y] = xj[0, ny + y]

            planes(0, w, stage)
            return [
                send(halo_out.at[e, 0], halo_in.at[e, 0], down),
                send(halo_out.at[e, 1], halo_in.at[e, 1], up),
            ]

        copies = None
        if sweep > 0:
            copies = send_halo(exchanges)

        def forces(y):
            u, v = x[0, y + 1], x[1, y + 1]
            feed, kill = f_ref[y], k_ref[y]
            uvv = u * v * v
            react = (feed * (1.0 - u) - uvv, uvv - (feed + kill) * v)
            for a, value in enumerate((u, v)):
                low = edge_in[sweep, 0, a, pl.ds(y, 1), :]
                high = edge_in[sweep, 1, a, pl.ds(y, 1), :]
                total = x[a, y] + x[a, y + 2]
                total = total + jnp.where(row == 0, low, pltpu.roll(value, 1, 0))
                total = total + jnp.where(row == nx - 1, high, pltpu.roll(value, nx - 1, 0))
                total = total + pltpu.roll(value, 1, 1) + pltpu.roll(value, nz - 1, 1)
                d = diffusion_values[a] * (total - 6.0 * value)
                diff[a, y] = d
                force[sweep, a, y] = d + react[a]

        order = [0, CHUNKS - 1] + list(range(1, CHUNKS - 1))
        core_copies, part_copies, right_copies = {}, {}, {}
        for c in order:
            rows = pl.ds(c * step, step)
            planes(c * step, (c + 1) * step, forces)
            core_copies[c] = send(
                force.at[sweep, :, rows], force_in.at[sweep, :, rows], core
            )
        if sweep == 0:
            start_copy.wait_recv()

            def begin(y):
                for a in range(2):
                    first = jnp.where(lax.rem(m, 2) == 1, x_ref[a, y], start[a, y])
                    start_kept[a, y] = has_start * first

            start_kept = local.at[1]
            planes(0, ny, begin)
        start_kept = local.at[1]

        def parts(y):
            for a in range(2):
                f, g, begin_value = force[sweep, a, y], force_in[sweep, a, y], start_kept[a, y]
                part_out[sweep, a, y] = begin_value + p_own * f + p_core * g
                local[0, a, y] = begin_value + q_own * f + q_core * g - (h * tau) * diff[a, y]

        for c in order:
            rows = pl.ds(c * step, step)
            core_copies[c].wait_recv()
            planes(c * step, (c + 1) * step, parts)
            part_copies[c] = send(
                part_out.at[sweep, :, rows], part_in.at[sweep, :, rows], across
            )

        if sweep == 0:
            first_pair.wait_recv()
            copies = send_halo(exchanges)

        scale_own = jnp.where(s == 0, scale[0], scale[1])
        scale_other = jnp.where(s == 0, scale[1], scale[0])

        def rights(y):
            rj[sweep, y + w, own_rows, :] = (local[0, s, y] + part_in[sweep, s, y]) * scale_own
            right_out[sweep, y] = (local[0, other, y] + part_in[sweep, other, y]) * scale_other

        near = min(step, w - 1)
        far = w - 1 - near
        right_halo = []

        def send_right(low, high, many):
            right_halo.append(send(
                rj.at[sweep, pl.ds(w + low, many)], rj.at[sweep, pl.ds(w + ny + low, many)], down
            ))
            right_halo.append(send(
                rj.at[sweep, pl.ds(w + high, many)], rj.at[sweep, pl.ds(w + high - ny, many)], up
            ))

        for place, c in enumerate(order):
            if place == 2:
                for done in order[:2]:
                    right_copies[done].wait_recv()
                send_right(0, ny - near, near)
            part_copies[c].wait_recv()
            planes(c * step, (c + 1) * step, rights)
            right_copies[c] = send(
                right_out.at[sweep, pl.ds(c * step, step)],
                rj.at[sweep, pl.ds(w + c * step, step), own_rows, :],
                pair,
            )
        for c in order[2:]:
            right_copies[c].wait_recv()
        if far:
            send_right(near, ny - near - far, far)
        for block in range(JACOBI // w):
            e = exchanges
            exchanges += 1
            if block > 0:
                copies = send_halo(e)

            def sweep_planes(turn, first, last):
                src, dst = (turn - 1) % 2, turn % 2

                def one(y):
                    value = xj[src, y]
                    total = xj[src, y - 1] + xj[src, y + 1]
                    total = total + pltpu.roll(value, 1, 0) + pltpu.roll(value, full - 1, 0)
                    total = total + pltpu.roll(value, 1, 1) + pltpu.roll(value, nz - 1, 1)
                    xj[dst, y] = rj[sweep, y] + gain * total

                planes(first + w, last + w, one)

            for turn in range(1, w + 1):
                sweep_planes(turn, turn, ny - turn)
            for copy in copies:
                copy.wait_recv()
            if block == 0:
                for copy in right_halo:
                    copy.wait_recv()

            def land(y):
                xj[0, w + ny + y] = halo_in[e, 0, y]
                xj[0, y] = halo_in[e, 1, y]

            planes(0, w, land)
            for turn in range(1, w + 1):
                sweep_planes(turn, turn - w, turn)
                sweep_planes(turn, ny - turn, ny + w - turn)
        source = xj.at[0, pl.ds(w, ny), other_rows, :]
        if sweep < SWEEPS - 1:
            copy = send(source, xe.at[sweep + 1, s, pl.ds(1, ny)], pair)

            def keep(y):
                xe[sweep + 1, s, y + 1] = xj[0, y + w, own_rows, :]

            planes(0, ny, keep)
            copy.wait_recv()
            copy.wait_send()
            started.pop()
        else:
            copy = send(source, back, pair)

            def keep(y):
                out_ref[s, y] = xj[0, y + w, own_rows, :]

            planes(0, ny, keep)
            copy.wait_recv()

            def finish(y):
                out_ref[other, y] = back[y]

            planes(0, ny, finish)
    for copy in started:
        copy.wait_send()


def fast_body(sy_count, previous, feed_rate, kill_rate):
    f32 = jnp.float32
    x = jnp.swapaxes(previous[0], 1, 2)
    _, ny, nx, nz = x.shape
    w = WIDTH
    block = (2, ny, nx, nz)
    blocks = SWEEPS * (JACOBI // w)
    copies = SWEEPS * (4 + 3 * CHUNKS + 4 + 2 * (JACOBI // w) + 1) + 2
    vmem = pl.BlockSpec(memory_space=pltpu.VMEM)
    out = pl.pallas_call(
        lambda *refs: kernel(sy_count, *refs),
        out_shape=jax.ShapeDtypeStruct(block, f32),
        in_specs=[vmem] * 3,
        out_specs=vmem,
        scratch_shapes=[
            pltpu.VMEM((SWEEPS, 2, ny + 2, nx, nz), f32),
            pltpu.VMEM((SWEEPS, 2, 2, ny, nz), f32),
            pltpu.VMEM((SWEEPS, 2, 2, ny, nz), f32),
            pltpu.VMEM(block, f32),
            pltpu.VMEM((SWEEPS,) + block, f32),
            pltpu.VMEM((SWEEPS,) + block, f32),
            pltpu.VMEM(block, f32),
            pltpu.VMEM((SWEEPS,) + block, f32),
            pltpu.VMEM((SWEEPS,) + block, f32),
            pltpu.VMEM((2,) + block, f32),
            pltpu.VMEM((SWEEPS, ny, nx, nz), f32),
            pltpu.VMEM((SWEEPS, ny + 2 * w, 2 * nx, nz), f32),
            pltpu.VMEM((2, ny + 2 * w, 2 * nx, nz), f32),
            pltpu.VMEM((blocks, 2, w, 2 * nx, nz), f32),
            pltpu.VMEM((blocks, 2, w, 2 * nx, nz), f32),
            pltpu.VMEM((ny, nx, nz), f32),
            pltpu.SemaphoreType.DMA((copies,)),
            pltpu.SemaphoreType.DMA((copies,)),
        ],
        compiler_params=pltpu.CompilerParams(
            collective_id=0, has_side_effects=True, vmem_limit_bytes=48 * 1024 * 1024
        ),
    )(x, jnp.swapaxes(feed_rate, 0, 1), jnp.swapaxes(kill_rate, 0, 1))
    return jnp.swapaxes(out, 1, 2)[None]


def solution(mesh):
    sizes = dict(mesh.shape)
    fast = sizes["sx"] == 2 and sizes["node"] == len(radau_points) and sizes["sy"] > 2

    def run(previous, feed_rate, kill_rate):
        if fast:
            return fast_body(sizes["sy"], previous, feed_rate, kill_rate)
        return body(previous, feed_rate, kill_rate)

    return jax.shard_map(
        run,
        mesh=mesh,
        in_specs=(P("node", None, "sx", "sy", None), P("sx", "sy", None), P("sx", "sy", None)),
        out_specs=P("node", None, "sx", "sy", None),
        check_vma=False,
    )
```

```python
import jax
import jax.numpy as jnp
from jax import lax
from jax.experimental import pallas as pl
from jax.experimental.pallas import tpu as pltpu
from jax.sharding import PartitionSpec as P

MESH = pl.DeviceIdType.MESH
WIDTH = 12
CHUNKS = 4
GROUP = 4

SWEEPS = 2
JACOBI = 12


radau_points = [0.088587959512704, 0.409466864440735, 0.787659461760847, 1.0]
time_step = 4.0
diffusion_values = [1.0, 0.5]


def from_root(value, axis, source):
    kept = jnp.where(lax.axis_index(axis) == source, value, 0).astype(value.dtype)
    return lax.psum(kept, axis)


def padded_2(block, sides, width):
    for axis, dim in sides:
        count = lax.axis_size(axis)
        forward = [(i, i + 1) for i in range(count - 1)]
        forward.append((count - 1, 0))
        backward = [(target, source) for source, target in forward]
        low = lax.ppermute(
            lax.slice_in_dim(block, block.shape[dim] - width, None, axis=dim), axis, forward
        )
        high = lax.ppermute(lax.slice_in_dim(block, 0, width, axis=dim), axis, backward)
        block = jnp.concatenate([low, block, high], axis=dim)
    return block


def collocation():
    count = len(radau_points)
    table = []
    for row in range(count):
        table.append([0.0] * count)
    for column in range(count):
        poly = [1.0]
        denom = 1.0
        for other in range(count):
            if other != column:
                longer = [0.0] * (len(poly) + 1)
                for place in range(len(poly)):
                    longer[place + 1] = longer[place + 1] + poly[place]
                    longer[place] = longer[place] - radau_points[other] * poly[place]
                poly = longer
                denom = denom * (radau_points[column] - radau_points[other])
        for row in range(count):
            point = radau_points[row]
            total = 0.0
            for place in range(len(poly)):
                total = total + poly[place] * point ** (place + 1) / (place + 1)
            table[row][column] = total / denom
    return table


def beside(padded):
    center = padded[:, 1:-1, 1:-1]
    total = padded[:, 2:, 1:-1] + padded[:, :-2, 1:-1]
    total = total + padded[:, 1:-1, 2:] + padded[:, 1:-1, :-2]
    return total + jnp.roll(center, 1, 3) + jnp.roll(center, -1, 3)


def body(previous, feed_rate, kill_rate):
    node_index = lax.axis_index("node")
    qmatrix = jnp.asarray(collocation(), jnp.float32)
    points = jnp.asarray(radau_points, jnp.float32)
    diag_weight = points[node_index]
    diffusion = jnp.asarray(diffusion_values, jnp.float32)[:, None, None, None]
    coef = time_step * diag_weight * diffusion
    start_value = from_root(previous[0], "node", len(radau_points) - 1)
    iterate = previous[0]
    for sweep in range(SWEEPS):
        padded = padded_2(iterate, (("sx", 1), ("sy", 2)), 1)
        diff = diffusion * (beside(padded) - 6.0 * iterate)
        upart = iterate[0]
        vpart = iterate[1]
        uvv = upart * vpart * vpart
        react = jnp.stack(
            [-uvv + feed_rate * (1.0 - upart), uvv - (feed_rate + kill_rate) * vpart], 0
        )
        force = diff + react
        weights = qmatrix[:, node_index][:, None, None, None, None]
        section_terms = weights * force[None]
        summed = lax.psum_scatter(section_terms, "node", scatter_dimension=0, tiled=True)[0]
        right_side = start_value + time_step * (summed - diag_weight * diff)
        extended = padded_2(right_side, (("sx", 1), ("sy", 2)), 1)

        def double_turn(turn, current):
            beside_all = padded_2(current, (("sx", 1), ("sy", 2)), 2)
            midway = (extended + coef * beside(beside_all)) / (1.0 + 6.0 * coef)
            return (right_side + coef * beside(midway)) / (1.0 + 6.0 * coef)

        iterate = lax.fori_loop(0, JACOBI // 2, double_turn, iterate)
    return iterate[None]


def pick(values, index):
    out = jnp.float32(values[-1])
    for at in range(len(values) - 1):
        out = jnp.where(index == at, jnp.float32(values[at]), out)
    return out


def pick_pair(table, row, column):
    out = pick(table[-1], column)
    for at in range(len(table) - 1):
        out = jnp.where(row == at, pick(table[at], column), out)
    return out


def kernel(
    sy_count, x_ref, f_ref, k_ref, out_ref,
    xe, edge_out, edge_in, diff, force, force_in, start, part_out, part_in,
    local, right_out, rj, xj, halo_out, halo_in, back, send_sems, recv_sems,
):
    w = WIDTH
    _, ny, nx, nz = x_ref.shape
    full = 2 * nx
    step = ny // CHUNKS
    m, s, t = lax.axis_index("node"), lax.axis_index("sx"), lax.axis_index("sy")
    other = 1 - s
    core = {"node": m + 1 - 2 * lax.rem(m, 2)}
    across = {"node": lax.rem(m + 2, 4)}
    pair = {"sx": other}
    up = {"sy": lax.rem(t + 1, sy_count)}
    down = {"sy": lax.rem(t + sy_count - 1, sy_count)}
    m1, m2 = core["node"], across["node"]
    count = [0]

    def send(src, dst, target):
        at = count[0]
        count[0] += 1
        copy = pltpu.make_async_remote_copy(
            src_ref=src, dst_ref=dst, send_sem=send_sems.at[at], recv_sem=recv_sems.at[at],
            device_id=target, device_id_type=MESH,
        )
        copy.start()
        started.append(copy)
        return copy

    started = []
    barrier = pltpu.get_barrier_semaphore()
    for target in (core, across, pair, up, down):
        pl.semaphore_signal(barrier, inc=1, device_id=target, device_id_type=MESH)

    table = collocation()
    h = time_step
    q_own, q_core = h * pick_pair(table, m, m), h * pick_pair(table, m, m1)
    p_own, p_core = h * pick_pair(table, m2, m), h * pick_pair(table, m2, m1)
    tau = pick(radau_points, m)
    has_start = jnp.where(m >= 2, jnp.float32(1.0), jnp.float32(0.0))
    scale = [1.0 / (1.0 + 6.0 * h * tau * d) for d in diffusion_values]
    coef_s = h * tau * pick(diffusion_values, s)
    gain = coef_s / (1.0 + 6.0 * coef_s)
    own_rows = pl.ds(pl.multiple_of(nx * s, nx), nx)
    other_rows = pl.ds(pl.multiple_of(nx * other, nx), nx)
    row = lax.broadcasted_iota(jnp.int32, (nx, nz), 0)

    def groups(first, last, fn):
        whole = (last - first) // GROUP

        def go(at, carry):
            fn(first + at * GROUP, GROUP)
            return carry

        if whole > 0:
            lax.fori_loop(0, whole, go, 0)
        rest = (last - first) - whole * GROUP
        if rest > 0:
            fn(first + whole * GROUP, rest)

    def planes(first, last, fn):
        def some(y, many):
            for at in range(many):
                fn(y + at)

        groups(first, last, some)

    def load(y):
        for a in range(2):
            xe[0, a, y + 1] = x_ref[a, y]
        xj[0, y + w, own_rows, :] = x_ref[s, y]

    planes(0, ny, load)
    pl.semaphore_wait(barrier, 5)

    exchanges = 0
    first_pair = None
    for sweep in range(SWEEPS):
        x = xe.at[sweep]

        def edges(y):
            for a in range(2):
                edge_out[sweep, 0, a, pl.ds(y, 1), :] = x[a, y + 1, pl.ds(0, 1), :]
                edge_out[sweep, 1, a, pl.ds(y, 1), :] = x[a, y + 1, pl.ds(nx - 1, 1), :]

        edge_copies = [
            send(x.at[:, ny], x.at[:, 0], up),
            send(x.at[:, 1], x.at[:, ny + 1], down),
        ]
        planes(0, ny, edges)
        edge_copies += [
            send(edge_out.at[sweep, 1], edge_in.at[sweep, 0], pair),
            send(edge_out.at[sweep, 0], edge_in.at[sweep, 1], pair),
        ]
        start_copy = None
        if sweep == 0:
            start_copy = send(x_ref, start, core)
            first_pair = send(x_ref.at[other], xj.at[0, pl.ds(w, ny), own_rows, :], pair)
        for copy in edge_copies:
            copy.wait_recv()

        def send_halo(e):
            def stage(y):
                halo_out[e, 0, y] = xj[0, w + y]
                halo_out[e, 1, y] = xj[0, ny + y]

            planes(0, w, stage)
            return [
                send(halo_out.at[e, 0], halo_in.at[e, 0], down),
                send(halo_out.at[e, 1], halo_in.at[e, 1], up),
            ]

        copies = None
        if sweep > 0:
            copies = send_halo(exchanges)

        def forces(y):
            u, v = x[0, y + 1], x[1, y + 1]
            feed, kill = f_ref[y], k_ref[y]
            uvv = u * v * v
            react = (feed * (1.0 - u) - uvv, uvv - (feed + kill) * v)
            for a, value in enumerate((u, v)):
                low = edge_in[sweep, 0, a, pl.ds(y, 1), :]
                high = edge_in[sweep, 1, a, pl.ds(y, 1), :]
                total = x[a, y] + x[a, y + 2]
                total = total + jnp.where(row == 0, low, pltpu.roll(value, 1, 0))
                total = total + jnp.where(row == nx - 1, high, pltpu.roll(value, nx - 1, 0))
                total = total + pltpu.roll(value, 1, 1) + pltpu.roll(value, nz - 1, 1)
                d = diffusion_values[a] * (total - 6.0 * value)
                diff[a, y] = d
                force[sweep, a, y] = d + react[a]

        order = [0, CHUNKS - 1] + list(range(1, CHUNKS - 1))
        core_copies, part_copies, right_copies = {}, {}, {}
        for c in order:
            rows = pl.ds(c * step, step)
            planes(c * step, (c + 1) * step, forces)
            core_copies[c] = send(
                force.at[sweep, :, rows], force_in.at[sweep, :, rows], core
            )
        if sweep == 0:
            start_copy.wait_recv()

            def begin(y):
                for a in range(2):
                    first = jnp.where(lax.rem(m, 2) == 1, x_ref[a, y], start[a, y])
                    start_kept[a, y] = has_start * first

            start_kept = local.at[1]
            planes(0, ny, begin)
        start_kept = local.at[1]

        def parts(y):
            for a in range(2):
                f, g, begin_value = force[sweep, a, y], force_in[sweep, a, y], start_kept[a, y]
                part_out[sweep, a, y] = begin_value + p_own * f + p_core * g
                local[0, a, y] = begin_value + q_own * f + q_core * g - (h * tau) * diff[a, y]

        for c in order:
            rows = pl.ds(c * step, step)
            core_copies[c].wait_recv()
            planes(c * step, (c + 1) * step, parts)
            part_copies[c] = send(
                part_out.at[sweep, :, rows], part_in.at[sweep, :, rows], across
            )

        if sweep == 0:
            first_pair.wait_recv()
            copies = send_halo(exchanges)

        scale_own = jnp.where(s == 0, scale[0], scale[1])
        scale_other = jnp.where(s == 0, scale[1], scale[0])

        def rights(y):
            rj[sweep, y + w, own_rows, :] = (local[0, s, y] + part_in[sweep, s, y]) * scale_own
            right_out[sweep, y] = (local[0, other, y] + part_in[sweep, other, y]) * scale_other

        near = min(step, w - 1)
        far = w - 1 - near
        right_halo = []

        def send_right(low, high, many):
            right_halo.append(send(
                rj.at[sweep, pl.ds(w + low, many)], rj.at[sweep, pl.ds(w + ny + low, many)], down
            ))
            right_halo.append(send(
                rj.at[sweep, pl.ds(w + high, many)], rj.at[sweep, pl.ds(w + high - ny, many)], up
            ))

        for place, c in enumerate(order):
            if place == 2:
                for done in order[:2]:
                    right_copies[done].wait_recv()
                send_right(0, ny - near, near)
            part_copies[c].wait_recv()
            planes(c * step, (c + 1) * step, rights)
            right_copies[c] = send(
                right_out.at[sweep, pl.ds(c * step, step)],
                rj.at[sweep, pl.ds(w + c * step, step), own_rows, :],
                pair,
            )
        for c in order[2:]:
            right_copies[c].wait_recv()
        if far:
            send_right(near, ny - near - far, far)
        for block in range(JACOBI // w):
            e = exchanges
            exchanges += 1
            if block > 0:
                copies = send_halo(e)

            def sweep_planes(turn, first, last):
                src, dst = (turn - 1) % 2, turn % 2

                def some(y, many):
                    held = [xj[src, y + at] for at in range(-1, many + 1)]
                    results = []
                    for at in range(many):
                        value = held[at + 1]
                        total = held[at] + held[at + 2]
                        total = total + pltpu.roll(value, 1, 0) + pltpu.roll(value, full - 1, 0)
                        total = total + pltpu.roll(value, 1, 1) + pltpu.roll(value, nz - 1, 1)
                        results.append(rj[sweep, y + at] + gain * total)
                    for at in range(many):
                        xj[dst, y + at] = results[at]

                groups(first + w, last + w, some)

            for turn in range(1, w + 1):
                sweep_planes(turn, turn, ny - turn)
            for copy in copies:
                copy.wait_recv()
            if block == 0:
                for copy in right_halo:
                    copy.wait_recv()

            def land(y):
                xj[0, w + ny + y] = halo_in[e, 0, y]
                xj[0, y] = halo_in[e, 1, y]

            planes(0, w, land)
            for turn in range(1, w + 1):
                sweep_planes(turn, turn - w, turn)
                sweep_planes(turn, ny - turn, ny + w - turn)
        source = xj.at[0, pl.ds(w, ny), other_rows, :]
        if sweep < SWEEPS - 1:
            copy = send(source, xe.at[sweep + 1, s, pl.ds(1, ny)], pair)

            def keep(y):
                xe[sweep + 1, s, y + 1] = xj[0, y + w, own_rows, :]

            planes(0, ny, keep)
            copy.wait_recv()
            copy.wait_send()
            started.pop()
        else:
            copy = send(source, back, pair)

            def keep(y):
                out_ref[s, y] = xj[0, y + w, own_rows, :]

            planes(0, ny, keep)
            copy.wait_recv()

            def finish(y):
                out_ref[other, y] = back[y]

            planes(0, ny, finish)
    for copy in started:
        copy.wait_send()


def fast_body(sy_count, previous, feed_rate, kill_rate):
    f32 = jnp.float32
    x = jnp.swapaxes(previous[0], 1, 2)
    _, ny, nx, nz = x.shape
    w = WIDTH
    block = (2, ny, nx, nz)
    blocks = SWEEPS * (JACOBI // w)
    copies = SWEEPS * (4 + 3 * CHUNKS + 4 + 2 * (JACOBI // w) + 1) + 2
    vmem = pl.BlockSpec(memory_space=pltpu.VMEM)
    out = pl.pallas_call(
        lambda *refs: kernel(sy_count, *refs),
        out_shape=jax.ShapeDtypeStruct(block, f32),
        in_specs=[vmem] * 3,
        out_specs=vmem,
        scratch_shapes=[
            pltpu.VMEM((SWEEPS, 2, ny + 2, nx, nz), f32),
            pltpu.VMEM((SWEEPS, 2, 2, ny, nz), f32),
            pltpu.VMEM((SWEEPS, 2, 2, ny, nz), f32),
            pltpu.VMEM(block, f32),
            pltpu.VMEM((SWEEPS,) + block, f32),
            pltpu.VMEM((SWEEPS,) + block, f32),
            pltpu.VMEM(block, f32),
            pltpu.VMEM((SWEEPS,) + block, f32),
            pltpu.VMEM((SWEEPS,) + block, f32),
            pltpu.VMEM((2,) + block, f32),
            pltpu.VMEM((SWEEPS, ny, nx, nz), f32),
            pltpu.VMEM((SWEEPS, ny + 2 * w, 2 * nx, nz), f32),
            pltpu.VMEM((2, ny + 2 * w, 2 * nx, nz), f32),
            pltpu.VMEM((blocks, 2, w, 2 * nx, nz), f32),
            pltpu.VMEM((blocks, 2, w, 2 * nx, nz), f32),
            pltpu.VMEM((ny, nx, nz), f32),
            pltpu.SemaphoreType.DMA((copies,)),
            pltpu.SemaphoreType.DMA((copies,)),
        ],
        compiler_params=pltpu.CompilerParams(
            collective_id=0, has_side_effects=True, vmem_limit_bytes=48 * 1024 * 1024
        ),
    )(x, jnp.swapaxes(feed_rate, 0, 1), jnp.swapaxes(kill_rate, 0, 1))
    return jnp.swapaxes(out, 1, 2)[None]


def solution(mesh):
    sizes = dict(mesh.shape)
    fast = sizes["sx"] == 2 and sizes["node"] == len(radau_points) and sizes["sy"] > 2

    def run(previous, feed_rate, kill_rate):
        if fast:
            return fast_body(sizes["sy"], previous, feed_rate, kill_rate)
        return body(previous, feed_rate, kill_rate)

    return jax.shard_map(
        run,
        mesh=mesh,
        in_specs=(P("node", None, "sx", "sy", None), P("sx", "sy", None), P("sx", "sy", None)),
        out_specs=P("node", None, "sx", "sy", None),
        check_vma=False,
    )
```

```python
import jax
import jax.numpy as jnp
from jax import lax
from jax.experimental import pallas as pl
from jax.experimental.pallas import tpu as pltpu
from jax.sharding import PartitionSpec as P

MESH = pl.DeviceIdType.MESH
WIDTH = 12
CHUNKS = 4
GROUP = 4

SWEEPS = 2
JACOBI = 12


radau_points = [0.088587959512704, 0.409466864440735, 0.787659461760847, 1.0]
time_step = 4.0
diffusion_values = [1.0, 0.5]


def from_root(value, axis, source):
    kept = jnp.where(lax.axis_index(axis) == source, value, 0).astype(value.dtype)
    return lax.psum(kept, axis)


def padded_2(block, sides, width):
    for axis, dim in sides:
        count = lax.axis_size(axis)
        forward = [(i, i + 1) for i in range(count - 1)]
        forward.append((count - 1, 0))
        backward = [(target, source) for source, target in forward]
        low = lax.ppermute(
            lax.slice_in_dim(block, block.shape[dim] - width, None, axis=dim), axis, forward
        )
        high = lax.ppermute(lax.slice_in_dim(block, 0, width, axis=dim), axis, backward)
        block = jnp.concatenate([low, block, high], axis=dim)
    return block


def collocation():
    count = len(radau_points)
    table = []
    for row in range(count):
        table.append([0.0] * count)
    for column in range(count):
        poly = [1.0]
        denom = 1.0
        for other in range(count):
            if other != column:
                longer = [0.0] * (len(poly) + 1)
                for place in range(len(poly)):
                    longer[place + 1] = longer[place + 1] + poly[place]
                    longer[place] = longer[place] - radau_points[other] * poly[place]
                poly = longer
                denom = denom * (radau_points[column] - radau_points[other])
        for row in range(count):
            point = radau_points[row]
            total = 0.0
            for place in range(len(poly)):
                total = total + poly[place] * point ** (place + 1) / (place + 1)
            table[row][column] = total / denom
    return table


def beside(padded):
    center = padded[:, 1:-1, 1:-1]
    total = padded[:, 2:, 1:-1] + padded[:, :-2, 1:-1]
    total = total + padded[:, 1:-1, 2:] + padded[:, 1:-1, :-2]
    return total + jnp.roll(center, 1, 3) + jnp.roll(center, -1, 3)


def body(previous, feed_rate, kill_rate):
    node_index = lax.axis_index("node")
    qmatrix = jnp.asarray(collocation(), jnp.float32)
    points = jnp.asarray(radau_points, jnp.float32)
    diag_weight = points[node_index]
    diffusion = jnp.asarray(diffusion_values, jnp.float32)[:, None, None, None]
    coef = time_step * diag_weight * diffusion
    start_value = from_root(previous[0], "node", len(radau_points) - 1)
    iterate = previous[0]
    for sweep in range(SWEEPS):
        padded = padded_2(iterate, (("sx", 1), ("sy", 2)), 1)
        diff = diffusion * (beside(padded) - 6.0 * iterate)
        upart = iterate[0]
        vpart = iterate[1]
        uvv = upart * vpart * vpart
        react = jnp.stack(
            [-uvv + feed_rate * (1.0 - upart), uvv - (feed_rate + kill_rate) * vpart], 0
        )
        force = diff + react
        weights = qmatrix[:, node_index][:, None, None, None, None]
        section_terms = weights * force[None]
        summed = lax.psum_scatter(section_terms, "node", scatter_dimension=0, tiled=True)[0]
        right_side = start_value + time_step * (summed - diag_weight * diff)
        extended = padded_2(right_side, (("sx", 1), ("sy", 2)), 1)

        def double_turn(turn, current):
            beside_all = padded_2(current, (("sx", 1), ("sy", 2)), 2)
            midway = (extended + coef * beside(beside_all)) / (1.0 + 6.0 * coef)
            return (right_side + coef * beside(midway)) / (1.0 + 6.0 * coef)

        iterate = lax.fori_loop(0, JACOBI // 2, double_turn, iterate)
    return iterate[None]


def pick(values, index):
    out = jnp.float32(values[-1])
    for at in range(len(values) - 1):
        out = jnp.where(index == at, jnp.float32(values[at]), out)
    return out


def pick_pair(table, row, column):
    out = pick(table[-1], column)
    for at in range(len(table) - 1):
        out = jnp.where(row == at, pick(table[at], column), out)
    return out


def kernel(
    sy_count, x_ref, f_ref, k_ref, out_ref,
    xe, edge_out, edge_in, diff, force, force_in, start, part_out, part_in,
    local, right_out, rj, xj, halo_out, halo_in, back, send_sems, recv_sems,
):
    w = WIDTH
    _, ny, nx, nz = x_ref.shape
    full = 2 * nx
    step = ny // CHUNKS
    m, s, t = lax.axis_index("node"), lax.axis_index("sx"), lax.axis_index("sy")
    other = 1 - s
    core = {"node": m + 1 - 2 * lax.rem(m, 2)}
    across = {"node": lax.rem(m + 2, 4)}
    pair = {"sx": other}
    up = {"sy": lax.rem(t + 1, sy_count)}
    down = {"sy": lax.rem(t + sy_count - 1, sy_count)}
    m1, m2 = core["node"], across["node"]
    count = [0]

    def send(src, dst, target):
        at = count[0]
        count[0] += 1
        copy = pltpu.make_async_remote_copy(
            src_ref=src, dst_ref=dst, send_sem=send_sems.at[at], recv_sem=recv_sems.at[at],
            device_id=target, device_id_type=MESH,
        )
        copy.start()
        started.append(copy)
        return copy

    started = []
    barrier = pltpu.get_barrier_semaphore()
    for target in (core, across, pair, up, down):
        pl.semaphore_signal(barrier, inc=1, device_id=target, device_id_type=MESH)

    table = collocation()
    h = time_step
    q_own, q_core = h * pick_pair(table, m, m), h * pick_pair(table, m, m1)
    p_own, p_core = h * pick_pair(table, m2, m), h * pick_pair(table, m2, m1)
    tau = pick(radau_points, m)
    has_start = jnp.where(m >= 2, jnp.float32(1.0), jnp.float32(0.0))
    scale = [1.0 / (1.0 + 6.0 * h * tau * d) for d in diffusion_values]
    coef_s = h * tau * pick(diffusion_values, s)
    gain = coef_s / (1.0 + 6.0 * coef_s)
    own_rows = pl.ds(pl.multiple_of(nx * s, nx), nx)
    other_rows = pl.ds(pl.multiple_of(nx * other, nx), nx)
    row = lax.broadcasted_iota(jnp.int32, (nx, nz), 0)

    def groups(first, last, fn):
        whole = (last - first) // GROUP

        def go(at, carry):
            fn(first + at * GROUP, GROUP)
            return carry

        if whole > 0:
            lax.fori_loop(0, whole, go, 0)
        rest = (last - first) - whole * GROUP
        if rest > 0:
            fn(first + whole * GROUP, rest)

    def planes(first, last, fn):
        def some(y, many):
            for at in range(many):
                fn(y + at)

        groups(first, last, some)

    def load(y):
        for a in range(2):
            xe[0, a, y + 1] = x_ref[a, y]
        xj[0, y + w, own_rows, :] = x_ref[s, y]

    planes(0, ny, load)
    pl.semaphore_wait(barrier, 5)

    exchanges = 0
    first_pair = None
    for sweep in range(SWEEPS):
        x = xe.at[sweep]

        def edges(y):
            for a in range(2):
                edge_out[sweep, 0, a, pl.ds(y, 1), :] = x[a, y + 1, pl.ds(0, 1), :]
                edge_out[sweep, 1, a, pl.ds(y, 1), :] = x[a, y + 1, pl.ds(nx - 1, 1), :]

        edge_copies = [
            send(x.at[:, ny], x.at[:, 0], up),
            send(x.at[:, 1], x.at[:, ny + 1], down),
        ]
        planes(0, ny, edges)
        edge_copies += [
            send(edge_out.at[sweep, 1], edge_in.at[sweep, 0], pair),
            send(edge_out.at[sweep, 0], edge_in.at[sweep, 1], pair),
        ]
        start_copy = None
        if sweep == 0:
            start_copy = send(x_ref, start, core)
            first_pair = send(x_ref.at[other], xj.at[0, pl.ds(w, ny), own_rows, :], pair)
        for copy in edge_copies:
            copy.wait_recv()

        def send_halo(e):
            def stage(y):
                halo_out[e, 0, y] = xj[0, w + y]
                halo_out[e, 1, y] = xj[0, ny + y]

            planes(0, w, stage)
            return [
                send(halo_out.at[e, 0], halo_in.at[e, 0], down),
                send(halo_out.at[e, 1], halo_in.at[e, 1], up),
            ]

        copies = None
        if sweep > 0:
            copies = send_halo(exchanges)

        def forces(y):
            u, v = x[0, y + 1], x[1, y + 1]
            feed, kill = f_ref[y], k_ref[y]
            uvv = u * v * v
            react = (feed * (1.0 - u) - uvv, uvv - (feed + kill) * v)
            for a, value in enumerate((u, v)):
                low = edge_in[sweep, 0, a, pl.ds(y, 1), :]
                high = edge_in[sweep, 1, a, pl.ds(y, 1), :]
                total = x[a, y] + x[a, y + 2]
                total = total + jnp.where(row == 0, low, pltpu.roll(value, 1, 0))
                total = total + jnp.where(row == nx - 1, high, pltpu.roll(value, nx - 1, 0))
                total = total + pltpu.roll(value, 1, 1) + pltpu.roll(value, nz - 1, 1)
                d = diffusion_values[a] * (total - 6.0 * value)
                diff[a, y] = d
                force[sweep, a, y] = d + react[a]

        order = [0, CHUNKS - 1] + list(range(1, CHUNKS - 1))
        core_copies, part_copies, right_copies = {}, {}, {}
        for c in order:
            rows = pl.ds(c * step, step)
            planes(c * step, (c + 1) * step, forces)
            core_copies[c] = send(
                force.at[sweep, :, rows], force_in.at[sweep, :, rows], core
            )
        if sweep == 0:
            start_copy.wait_recv()

            def begin(y):
                for a in range(2):
                    first = jnp.where(lax.rem(m, 2) == 1, x_ref[a, y], start[a, y])
                    start_kept[a, y] = has_start * first

            start_kept = local.at[1]
            planes(0, ny, begin)
        start_kept = local.at[1]

        def parts(y):
            for a in range(2):
                f, g, begin_value = force[sweep, a, y], force_in[sweep, a, y], start_kept[a, y]
                part_out[sweep, a, y] = begin_value + p_own * f + p_core * g
                local[0, a, y] = begin_value + q_own * f + q_core * g - (h * tau) * diff[a, y]

        for c in order:
            rows = pl.ds(c * step, step)
            core_copies[c].wait_recv()
            planes(c * step, (c + 1) * step, parts)
            part_copies[c] = send(
                part_out.at[sweep, :, rows], part_in.at[sweep, :, rows], across
            )

        if sweep == 0:
            first_pair.wait_recv()
            copies = send_halo(exchanges)

        scale_own = jnp.where(s == 0, scale[0], scale[1])
        scale_other = jnp.where(s == 0, scale[1], scale[0])

        def rights(y):
            rj[sweep, y + w, own_rows, :] = (local[0, s, y] + part_in[sweep, s, y]) * scale_own
            right_out[sweep, y] = (local[0, other, y] + part_in[sweep, other, y]) * scale_other

        near = min(step, w - 1)
        far = w - 1 - near
        right_halo = []

        def send_right(low, high, many):
            right_halo.append(send(
                rj.at[sweep, pl.ds(w + low, many)], rj.at[sweep, pl.ds(w + ny + low, many)], down
            ))
            right_halo.append(send(
                rj.at[sweep, pl.ds(w + high, many)], rj.at[sweep, pl.ds(w + high - ny, many)], up
            ))

        for place, c in enumerate(order):
            if place == 2:
                for done in order[:2]:
                    right_copies[done].wait_recv()
                send_right(0, ny - near, near)
            part_copies[c].wait_recv()
            planes(c * step, (c + 1) * step, rights)
            right_copies[c] = send(
                right_out.at[sweep, pl.ds(c * step, step)],
                rj.at[sweep, pl.ds(w + c * step, step), own_rows, :],
                pair,
            )
        for c in order[2:]:
            right_copies[c].wait_recv()
        if far:
            send_right(near, ny - near - far, far)
        backs = []

        def send_back(low, many):
            source = xj.at[0, pl.ds(w + low, many), other_rows, :]
            if sweep < SWEEPS - 1:
                target = xe.at[sweep + 1, s, pl.ds(1 + low, many)]
            else:
                target = back.at[pl.ds(low, many)]
            backs.append((low, many, send(source, target, pair)))

        for block in range(JACOBI // w):
            e = exchanges
            exchanges += 1
            if block > 0:
                copies = send_halo(e)

            def sweep_planes(turn, first, last):
                src, dst = (turn - 1) % 2, turn % 2

                def some(y, many):
                    held = [xj[src, y + at] for at in range(-1, many + 1)]
                    results = []
                    for at in range(many):
                        value = held[at + 1]
                        total = held[at] + held[at + 2]
                        total = total + pltpu.roll(value, 1, 0) + pltpu.roll(value, full - 1, 0)
                        total = total + pltpu.roll(value, 1, 1) + pltpu.roll(value, nz - 1, 1)
                        results.append(rj[sweep, y + at] + gain * total)
                    for at in range(many):
                        xj[dst, y + at] = results[at]

                groups(first + w, last + w, some)

            for turn in range(1, w + 1):
                sweep_planes(turn, turn, ny - turn)
            last_block = block == JACOBI // w - 1
            if last_block and ny > 2 * w:
                send_back(w, ny - 2 * w)
            for copy in copies:
                copy.wait_recv()
            if block == 0:
                for copy in right_halo:
                    copy.wait_recv()

            def land(y):
                xj[0, w + ny + y] = halo_in[e, 0, y]
                xj[0, y] = halo_in[e, 1, y]

            planes(0, w, land)
            for turn in range(1, w + 1):
                sweep_planes(turn, turn - w, turn)
            if last_block:
                send_back(0, w)
            for turn in range(1, w + 1):
                sweep_planes(turn, ny - turn, ny + w - turn)
            if last_block:
                send_back(ny - w, w)
        if sweep < SWEEPS - 1:
            def keep(y):
                xe[sweep + 1, s, y + 1] = xj[0, y + w, own_rows, :]

            planes(0, ny, keep)
            for _, _, copy in backs:
                copy.wait_recv()
                copy.wait_send()
                started.pop()
        else:
            def keep(y):
                out_ref[s, y] = xj[0, y + w, own_rows, :]

            planes(0, ny, keep)

            def finish(y):
                out_ref[other, y] = back[y]

            for low, many, copy in backs:
                copy.wait_recv()
                planes(low, low + many, finish)
    for copy in started:
        copy.wait_send()


def fast_body(sy_count, previous, feed_rate, kill_rate):
    f32 = jnp.float32
    x = jnp.swapaxes(previous[0], 1, 2)
    _, ny, nx, nz = x.shape
    w = WIDTH
    block = (2, ny, nx, nz)
    blocks = SWEEPS * (JACOBI // w)
    copies = SWEEPS * (4 + 3 * CHUNKS + 4 + 2 * (JACOBI // w) + 3) + 2
    vmem = pl.BlockSpec(memory_space=pltpu.VMEM)
    out = pl.pallas_call(
        lambda *refs: kernel(sy_count, *refs),
        out_shape=jax.ShapeDtypeStruct(block, f32),
        in_specs=[vmem] * 3,
        out_specs=vmem,
        scratch_shapes=[
            pltpu.VMEM((SWEEPS, 2, ny + 2, nx, nz), f32),
            pltpu.VMEM((SWEEPS, 2, 2, ny, nz), f32),
            pltpu.VMEM((SWEEPS, 2, 2, ny, nz), f32),
            pltpu.VMEM(block, f32),
            pltpu.VMEM((SWEEPS,) + block, f32),
            pltpu.VMEM((SWEEPS,) + block, f32),
            pltpu.VMEM(block, f32),
            pltpu.VMEM((SWEEPS,) + block, f32),
            pltpu.VMEM((SWEEPS,) + block, f32),
            pltpu.VMEM((2,) + block, f32),
            pltpu.VMEM((SWEEPS, ny, nx, nz), f32),
            pltpu.VMEM((SWEEPS, ny + 2 * w, 2 * nx, nz), f32),
            pltpu.VMEM((2, ny + 2 * w, 2 * nx, nz), f32),
            pltpu.VMEM((blocks, 2, w, 2 * nx, nz), f32),
            pltpu.VMEM((blocks, 2, w, 2 * nx, nz), f32),
            pltpu.VMEM((ny, nx, nz), f32),
            pltpu.SemaphoreType.DMA((copies,)),
            pltpu.SemaphoreType.DMA((copies,)),
        ],
        compiler_params=pltpu.CompilerParams(
            collective_id=0, has_side_effects=True, vmem_limit_bytes=48 * 1024 * 1024
        ),
    )(x, jnp.swapaxes(feed_rate, 0, 1), jnp.swapaxes(kill_rate, 0, 1))
    return jnp.swapaxes(out, 1, 2)[None]


def solution(mesh):
    sizes = dict(mesh.shape)
    fast = sizes["sx"] == 2 and sizes["node"] == len(radau_points) and sizes["sy"] > 2

    def run(previous, feed_rate, kill_rate):
        if fast:
            return fast_body(sizes["sy"], previous, feed_rate, kill_rate)
        return body(previous, feed_rate, kill_rate)

    return jax.shard_map(
        run,
        mesh=mesh,
        in_specs=(P("node", None, "sx", "sy", None), P("sx", "sy", None), P("sx", "sy", None)),
        out_specs=P("node", None, "sx", "sy", None),
        check_vma=False,
    )
```
